32 devices in a mesh: rep: 2 (over z, core), dp: 16 (over x, y).
Axes of the slice: x: 4, y: 4, z: 1, core: 2. Of those that a mesh axis runs over, the one named last changes fastest.
The devices are a block of a 4x4x8 slice.
Arguments:
- g_w_gate: bfloat16 [32, 2, 1152, 4608], P(('rep', 'dp')), parts along dimension 0
- g_w_up: bfloat16 [32, 2, 1152, 4608], P(('rep', 'dp')), parts along dimension 0
- g_w_down: bfloat16 [32, 2, 4608, 1152], P(('rep', 'dp')), parts along dimension 0
- w_gate: bfloat16 [2, 1152, 4608], replicated
- w_up: bfloat16 [2, 1152, 4608], replicated
- w_down: bfloat16 [2, 4608, 1152], replicated
- m_w_gate: float32 [2, 1152, 4608], P(None, 'dp')
- m_w_up: float32 [2, 1152, 4608], P(None, 'dp')
- m_w_down: float32 [2, 4608, 1152], P(None, 'dp')
- v_w_gate: float32 [2, 1152, 4608], P(None, 'dp')
- v_w_up: float32 [2, 1152, 4608], P(None, 'dp')
- v_w_down: float32 [2, 4608, 1152], P(None, 'dp')
Outputs:
- output 1: bfloat16 [4, 1152, 4608], P('rep'), parts along dimension 0
- output 2: bfloat16 [4, 1152, 4608], P('rep'), parts along dimension 0
- output 3: bfloat16 [4, 4608, 1152], P('rep'), parts along dimension 0
- output 4: float32 [4, 1152, 4608], P('rep', 'dp'), parts along dimension 0
- output 5: float32 [4, 1152, 4608], P('rep', 'dp'), parts along dimension 0
- output 6: float32 [4, 4608, 1152], P('rep', 'dp'), parts along dimension 0
- output 7: float32 [4, 1152, 4608], P('rep', 'dp'), parts along dimension 0
- output 8: float32 [4, 1152, 4608], P('rep', 'dp'), parts along dimension 0
- output 9: float32 [4, 4608, 1152], P('rep', 'dp'), parts along dimension 0
There are 2 independent parts. The reference program is written for one: setup_inputs(seed, part) draws one part's arguments, and reference() takes and returns one part's arrays. A program takes and returns all parts, laid end to end along the dimension named above; an argument that names none is the same for every part.
All inputs are finite; a program needn't handle non-finite values.
Results may differ from the reference program's by a relative error of at most 0.022.
Values are sent between devices in bfloat16 or wider.
A program may use at most 768 MiB of HBM per device.

```python
import jax
import jax.numpy as jnp
from jax import lax

DEVICES = 16
D = 1152
FF = 4608
LAYERS = 2
NAMES = ("w_gate", "w_up", "w_down")
SHAPES = {"w_gate": (LAYERS, D, FF), "w_up": (LAYERS, D, FF), "w_down": (LAYERS, FF, D)}


def setup_inputs(seed: int = 0, part: int = 0) -> dict:
    kz, *keys = jax.random.split(jax.random.key(seed), 1 + 5 * len(NAMES))
    loud = 2.0 ** jax.random.uniform(kz, (), jnp.float32, -1.0, 1.0)
    drawn = {}
    for name, key, both in zip(NAMES, keys[:3], keys[3:6], strict=True):
        own = jax.random.normal(jax.random.fold_in(key, part), (DEVICES, *SHAPES[name]), jnp.float32)
        shared = jax.random.normal(jax.random.fold_in(both, part), SHAPES[name], jnp.float32)
        drawn["g_" + name] = (loud * (0.7 * shared / DEVICES + 0.7 * own * DEVICES**-0.5)).astype(jnp.bfloat16)
    for name, key in zip(NAMES, keys[6:9], strict=True):
        drawn[name] = (jax.random.normal(key, SHAPES[name], jnp.float32) * SHAPES[name][1] ** -0.5).astype(jnp.bfloat16)
    for name, key in zip(NAMES, keys[9:12], strict=True):
        drawn["m_" + name] = loud * 0.5 * jax.random.normal(key, SHAPES[name], jnp.float32)
    for name, key in zip(NAMES, keys[12:15], strict=True):
        drawn["v_" + name] = loud * loud * jax.random.uniform(key, SHAPES[name], jnp.float32, 0.5, 1.5)
    return drawn


def adamw(w, m, v, g):
    m = 0.9 * m + 0.1 * g
    v = 0.95 * v + 0.05 * g * g
    step = m * lax.rsqrt(v + 1e-8) + 0.1 * w
    return (w - 0.02 * step).astype(jnp.bfloat16), m, v


def reference(g_w_gate, g_w_up, g_w_down, w_gate, w_up, w_down, m_w_gate, m_w_up, m_w_down, v_w_gate, v_w_up, v_w_down):
    def total(terms):
        return lax.scan(lambda so_far, term: (so_far + term.astype(jnp.float32), None), jnp.zeros(terms.shape[1:], jnp.float32), terms)[0]

    gradients = [total(terms).astype(jnp.bfloat16).astype(jnp.float32) for terms in (g_w_gate, g_w_up, g_w_down)]
    new = [
        adamw(w.astype(jnp.float32), m, v, g)
        for w, m, v, g in zip((w_gate, w_up, w_down), (m_w_gate, m_w_up, m_w_down), (v_w_gate, v_w_up, v_w_down), gradients, strict=True)
    ]
    return tuple(one[which] for which in range(3) for one in new)
```

```python
import functools
import math

import jax
import jax.numpy as jnp
from jax import lax
from jax.experimental import pallas as pl
from jax.experimental.pallas import tpu as pltpu
from jax.sharding import PartitionSpec as P


MESH = pl.DeviceIdType.MESH
ANY = pl.BlockSpec(memory_space=pl.ANY)
VMEM = pl.BlockSpec(memory_space=pltpu.VMEM)
WEIGHTS = 3
COLORS = 4
SLOTS = 3
SMALL = 8


class Grid:
    def __init__(self, n):
        me = lax.axis_index("dp")
        self.n, self.x, self.y = n, lax.div(me, n), lax.rem(me, n)
        self.me = me

    def sign(self, c):
        return 1 if c % 2 == 0 else -1

    def first(self, c):
        return self.x if c < 2 else self.y

    def second(self, c):
        return self.y if c < 2 else self.x

    def back(self, at, c, steps):
        return lax.rem(at + (2 * self.n - self.sign(c) * steps), self.n)

    def on(self, c, second):
        along_x = (c < 2) != second
        x, y = self.x, self.y
        if along_x:
            x = self.back(x, c, -1)
        else:
            y = self.back(y, c, -1)
        return {"dp": x * self.n + y}


def slab(ref, wide, layer, c, first, cols):
    owners = (first, slice(None)) if c < 2 else (slice(None), first)
    if wide:
        return ref.at[(layer, *owners, slice(None), pl.ds(c * cols, cols))]
    return ref.at[(layer, *owners, c)]


def piece(ref, wide, layer, c, first, second, cols):
    owner = (first, second) if c < 2 else (second, first)
    if wide:
        return ref.at[(layer, *owner, slice(None), pl.ds(c * cols, cols))]
    return ref.at[(layer, *owner, c)]


def mine(ref, wide, layer, c, cols):
    return ref.at[layer, :, pl.ds(c * cols, cols)] if wide else ref.at[layer, c]


def moments(m, v, g):
    return 0.9 * m + 0.1 * g, 0.95 * v + 0.05 * g * g


def adamw(w, m, v, g):
    m, v = moments(m, v, g)
    step = m * lax.rsqrt(v + 1e-8) + 0.1 * w
    return (w - 0.02 * step).astype(jnp.bfloat16)


def exchange(n, layers, wides, *refs):
    g, w, m, v = (refs[i * WEIGHTS : (i + 1) * WEIGHTS] for i in range(4))
    refs = refs[4 * WEIGHTS :]
    whole, refs = refs[:WEIGHTS], refs[WEIGHTS:]
    far, refs = refs[: WEIGHTS * COLORS], refs[WEIGHTS * COLORS :]
    total, got1, got2, refs = *refs[:3], refs[3:]
    a, b, s, a2, b2, c2, s2, gb, wb, wo, mo, vo, refs = *refs[:12], refs[12:]
    send1, recv1, send2, recv2, gsend1, grecv1, gsend2, grecv2, la, lb, la2, lb2, lc2, lg, lw, lo = refs

    rows, cols = gb.shape[2:]
    here = Grid(n)
    units = [(k, layer) for k in range(WEIGHTS) for layer in range(layers)]
    U = len(units)
    colors = range(COLORS)

    barrier = pltpu.get_barrier_semaphore()
    for c in colors:
        pl.semaphore_signal(barrier, inc=1, device_id=here.on(c, False), device_id_type=MESH)
    pl.semaphore_wait(barrier, COLORS)

    def to(src, dst, send, recv, c, second):
        return pltpu.make_async_remote_copy(src, dst, send, recv, device_id=here.on(c, second), device_id_type=MESH)

    def g_slab(u, c, steps):
        k, layer = units[u]
        return slab(g[k], wides[k], layer, c, here.back(here.first(c), c, steps), cols)

    def g_piece(u, c, steps):
        k, layer = units[u]
        return piece(g[k], wides[k], layer, c, here.first(c), here.back(here.second(c), c, steps), cols)

    def w_slab(u, c, steps):
        k, layer = units[u]
        return slab(whole[k], wides[k], layer, c, here.back(here.first(c), c, steps), cols)

    def w_piece(u, c, steps):
        k, layer = units[u]
        return piece(whole[k], wides[k], layer, c, here.first(c), here.back(here.second(c), c, steps), cols)

    def hop1(t, u, c, src):
        return to(src, got1.at[c, t, u], send1.at[c, t, u], recv1.at[c, t, u], c, False)

    def hop2(t, u, c, src):
        return to(src, got2.at[c, t, u], send2.at[c, t, u], recv2.at[c, t, u], c, True)

    for u in range(U):
        for c in colors:
            hop1(0, u, c, g_slab(u, c, 1)).start()

    own = []
    for u, (k, layer) in enumerate(units):
        for c in colors:
            own.append(pltpu.make_async_copy(mine(m[k], wides[k], layer, c, cols), mo.at[c, u], lo.at[0, c, u]))
            own.append(pltpu.make_async_copy(mine(v[k], wides[k], layer, c, cols), vo.at[c, u], lo.at[1, c, u]))
            owner = piece(w[k], wides[k], layer, c, here.first(c), here.second(c), cols)
            own.append(pltpu.make_async_copy(owner, wo.at[c, u], lo.at[2, c, u]))

    def load_b(r, t, u, c):
        return pltpu.make_async_copy(g_slab(u, c, 1 + t), b.at[r % 2, c], lb.at[r % 2, c])

    rounds = [(t, u) for t in range(1, n - 1) for u in range(U)]
    for c in colors:
        load_b(0, *rounds[0], c).start()
    for copy in own:
        copy.start()
    for r, (t, u) in enumerate(rounds):
        loads = [pltpu.make_async_copy(got1.at[c, t - 1, u], a.at[c], la.at[c]) for c in colors]
        for c in colors:
            hop1(t - 1, u, c, got1.at[c, t - 1, u]).wait_recv()
            loads[c].start()
        if r + 1 < len(rounds):
            for c in colors:
                load_b(r + 1, *rounds[r + 1], c).start()
        slot = r % SLOTS
        for c in colors:
            loads[c].wait()
            load_b(r, t, u, c).wait()
            if r >= SLOTS:
                before = rounds[r - SLOTS]
                hop1(*before, c, s.at[slot, c]).wait_send()

            @pl.loop(0, n)
            def _(j):
                @pl.loop(0, rows, step=8)
                def _(i):
                    at = pl.ds(pl.multiple_of(i, 8), 8)
                    both = a[c, j, at, :].astype(jnp.float32) + b[r % 2, c, j, at, :].astype(jnp.float32)
                    s[slot, c, j, at, :] = both.astype(jnp.bfloat16)

        for c in colors:
            hop1(t, u, c, s.at[slot, c]).start()

    def load_b2(r, t, u, c):
        return pltpu.make_async_copy(g_piece(u, c, 1 + t), b2.at[r % 2, c], lb2.at[r % 2, c])

    def load_c2(r, t, u, c):
        return pltpu.make_async_copy(
            got1.at[c, n - 2, u, here.back(here.second(c), c, 1 + t)], c2.at[r % 2, c], lc2.at[r % 2, c]
        )

    def keep(u, c):
        return pltpu.make_async_copy(gb.at[c, u], total.at[c, u], lg.at[c, u])

    def place(u, c):
        return pltpu.make_async_copy(wb.at[c, u], w_piece(u, c, 0), lw.at[c, u])

    def gather1(t, u, c):
        return to(wb.at[c, u] if t == 0 else w_piece(u, c, t), w_piece(u, c, t), gsend1.at[c, t, u], grecv1.at[c, t, u], c, True)

    rounds = [(t, u) for t in range(n) for u in range(U)]
    for c in colors:
        load_b2(0, *rounds[0], c).start()
    for r, (t, u) in enumerate(rounds):
        par, slot = r % 2, r % SMALL
        for c in colors:
            if t == 0:
                hop1(n - 2, u, c, got1.at[c, n - 2, u]).wait_recv()
                load_c2(r, t, u, c).start()
            else:
                hop2(t - 1, u, c, got2.at[c, t - 1, u]).wait_recv()
                pltpu.make_async_copy(got2.at[c, t - 1, u], a2.at[c], la2.at[c]).start()
        if r + 1 < len(rounds):
            for c in colors:
                load_b2(r + 1, *rounds[r + 1], c).start()
                if rounds[r + 1][0] > 0:
                    load_c2(r + 1, *rounds[r + 1], c).start()
        for c in colors:
            load_b2(r, t, u, c).wait()
            load_c2(r, t, u, c).wait()
            if t > 0:
                pltpu.make_async_copy(got2.at[c, t - 1, u], a2.at[c], la2.at[c]).wait()
            if t < n - 1 and r >= SMALL:
                hop2(*rounds[r - SMALL], c, s2.at[slot, c]).wait_send()
            if t == n - 1:
                for copy in own[3 * (u * COLORS + c) : 3 * (u * COLORS + c) + 3]:
                    copy.wait()

            @pl.loop(0, rows, step=8)
            def _(i):
                at = pl.ds(pl.multiple_of(i, 8), 8)
                so_far = b2[par, c, at, :].astype(jnp.float32) + c2[par, c, at, :].astype(jnp.float32)
                if t > 0:
                    so_far = so_far + a2[c, at, :].astype(jnp.float32)
                summed = so_far.astype(jnp.bfloat16)
                if t < n - 1:
                    s2[slot, c, at, :] = summed
                else:
                    gb[c, u, at, :] = summed
                    wb[c, u, at, :] = adamw(
                        wo[c, u, at, :].astype(jnp.float32), mo[c, u, at, :], vo[c, u, at, :], summed.astype(jnp.float32)
                    )

        for c in colors:
            if t < n - 1:
                hop2(t, u, c, s2.at[slot, c]).start()
            else:
                gather1(0, u, c).start()
                place(u, c).start()
                keep(u, c).start()

    def got_piece(t, u, c):
        at = w_piece(u, c, 1 + t)
        return to(at, at, gsend1.at[c, t, u], grecv1.at[c, t, u], c, True)

    def gather2(t, u, c):
        k, layer = units[u]
        at = w_slab(u, c, t)
        there = at if t < n - 3 else far[k * COLORS + c].at[layer]
        return to(at, there, gsend2.at[c, t, u], grecv2.at[c, t, u], c, False)

    def got_slab(t, u, c):
        k, layer = units[u]
        at = w_slab(u, c, 1 + t) if t < n - 3 else far[k * COLORS + c].at[layer]
        return to(at, at, gsend2.at[c, t, u], grecv2.at[c, t, u], c, False)

    for t in range(1, n - 1):
        for u in range(U):
            for c in colors:
                got_piece(t - 1, u, c).wait_recv()
                gather1(t, u, c).start()
    for t in range(n - 2):
        for u in range(U):
            for c in colors:
                if t == 0:
                    place(u, c).wait()
                    got_piece(n - 2, u, c).wait_recv()
                else:
                    got_slab(t - 1, u, c).wait_recv()
                gather2(t, u, c).start()

    for u in range(U):
        for c in colors:
            keep(u, c).wait()
            hop1(0, u, c, g_slab(u, c, 1)).wait_send()
            for t in range(n - 1):
                gather1(t, u, c).wait_send()
            for t in range(n - 2):
                gather2(t, u, c).wait_send()
    for t, u in [(t, u) for t in range(1, n - 1) for u in range(U)][-SLOTS:]:
        for c in colors:
            hop1(t, u, c, s.at[0, c]).wait_send()
    first = len([1 for t, u in rounds if t < n - 1])
    waited = {rounds[r - SMALL] for r in range(SMALL, first)}
    for t, u in rounds[:first]:
        if (t, u) not in waited:
            for c in colors:
                hop2(t, u, c, s2.at[0, c]).wait_send()
    for u in range(U):
        for c in colors:
            got_slab(n - 3, u, c).wait_recv()


def spread(n, layers, wides, *refs):
    whole, refs = refs[:WEIGHTS], refs[WEIGHTS:]
    far, refs = refs[: WEIGHTS * COLORS], refs[WEIGHTS * COLORS :]
    out, (buf, load_sem, store_sem) = refs[:WEIGHTS], refs[WEIGHTS:]
    slots, cols = buf.shape[0], buf.shape[-1]
    here = Grid(n)
    jobs = []
    for k in range(WEIGHTS):
        for layer in range(layers):
            for c in range(COLORS):
                for t in range(n - 1):
                    at = here.back(here.first(c), c, t)
                    dst = slab(out[k], wides[k], layer, c, at, cols)
                    src = slab(whole[k], wides[k], layer, c, at, cols) if t < n - 2 else far[k * COLORS + c].at[layer]
                    jobs.append((src, dst))

    def load(i):
        return pltpu.make_async_copy(jobs[i][0], buf.at[i % slots], load_sem.at[i % slots])

    def store(i):
        return pltpu.make_async_copy(buf.at[i % slots], jobs[i][1], store_sem.at[i % slots])

    lag = slots // 2
    for i in range(len(jobs) + lag):
        if i < len(jobs):
            if i >= slots:
                store(i - slots).wait()
            load(i).start()
        if i >= lag:
            load(i - lag).wait()
            store(i - lag).start()
    for i in range(len(jobs) - slots, len(jobs)):
        store(i).wait()


def finish(n, layers, wide, *refs):
    last, (_, out, sem) = refs[:COLORS], refs[COLORS:]
    here = Grid(n)
    copies = []
    for layer in range(layers):
        for c in range(COLORS):
            at = here.back(here.first(c), c, n - 1)
            copies.append(
                pltpu.make_async_copy(last[c].at[layer], slab(out, wide, layer, c, at, last[c].shape[-1]), sem.at[layer, c])
            )
    for copy in copies:
        copy.start()
    for copy in copies:
        copy.wait()


def new_moments(g_ref, m_ref, v_ref, m_out, v_out):
    g = g_ref[0, 0].astype(jnp.float32)
    m, v = moments(m_ref[0], v_ref[0], g)
    m_out[0], v_out[0] = m, v


def solution(mesh):
    n = math.isqrt(mesh.shape["dp"])

    def step(*arrays):
        terms, weights, m, v = (arrays[i : i + WEIGHTS] for i in range(0, 4 * WEIGHTS, WEIGHTS))
        layers = m[0].shape[0]
        rows = min(one.shape[1] for one in m)
        cols = min(one.shape[2] for one in m)
        wides = [one.shape[2] != cols for one in m]
        units = WEIGHTS * layers

        def blocks(one, wide):
            return one.reshape((layers, n, n, rows, COLORS * cols) if wide else (layers, n, n, COLORS, rows, cols))

        def own(one, wide):
            return one if wide else one.reshape(layers, COLORS, rows, cols)

        views = [blocks(one[0], wide) for one, wide in zip(terms, wides, strict=True)]
        views += [blocks(one, wide) for one, wide in zip(weights, wides, strict=True)]
        views += [own(one, wide) for one, wide in zip(m + v, wides + wides, strict=True)]
        bf16, f32 = jnp.bfloat16, jnp.float32
        dma = pltpu.SemaphoreType.DMA
        whole_shape = [jax.ShapeDtypeStruct(one.shape, bf16) for one in views[WEIGHTS : 2 * WEIGHTS]]
        far_shape = [jax.ShapeDtypeStruct((layers, n, rows, cols), bf16)] * (WEIGHTS * COLORS)
        results = pl.pallas_call(
            functools.partial(exchange, n, layers, wides),
            out_shape=(
                *whole_shape,
                *far_shape,
                jax.ShapeDtypeStruct((COLORS, units, rows, cols), bf16),
                jax.ShapeDtypeStruct((COLORS, n - 1, units, n, rows, cols), bf16),
                jax.ShapeDtypeStruct((COLORS, n - 1, units, rows, cols), bf16),
            ),
            in_specs=[ANY] * len(views),
            out_specs=[ANY] * (WEIGHTS + WEIGHTS * COLORS + 3),
            scratch_shapes=[
                pltpu.VMEM((COLORS, n, rows, cols), bf16),
                pltpu.VMEM((2, COLORS, n, rows, cols), bf16),
                pltpu.VMEM((SLOTS, COLORS, n, rows, cols), bf16),
                pltpu.VMEM((COLORS, rows, cols), bf16),
                pltpu.VMEM((2, COLORS, rows, cols), bf16),
                pltpu.VMEM((2, COLORS, rows, cols), bf16),
                pltpu.VMEM((SMALL, COLORS, rows, cols), bf16),
                pltpu.VMEM((COLORS, units, rows, cols), bf16),
                pltpu.VMEM((COLORS, units, rows, cols), bf16),
                pltpu.VMEM((COLORS, units, rows, cols), bf16),
                pltpu.VMEM((COLORS, units, rows, cols), f32),
                pltpu.VMEM((COLORS, units, rows, cols), f32),
                dma((COLORS, n - 1, units)),
                dma((COLORS, n - 1, units)),
                dma((COLORS, n - 1, units)),
                dma((COLORS, n - 1, units)),
                dma((COLORS, n - 1, units)),
                dma((COLORS, n - 1, units)),
                dma((COLORS, n - 2, units)),
                dma((COLORS, n - 2, units)),
                dma((COLORS,)),
                dma((2, COLORS)),
                dma((COLORS,)),
                dma((2, COLORS)),
                dma((2, COLORS)),
                dma((COLORS, units)),
                dma((COLORS, units)),
                dma((3, COLORS, units)),
            ],
            compiler_params=pltpu.CompilerParams(collective_id=0, has_side_effects=True, vmem_limit_bytes=62 << 20),
            name="exchange",
        )(*views)
        whole, far, total = results[:WEIGHTS], results[WEIGHTS : WEIGHTS + WEIGHTS * COLORS], results[-3]

        def along(c):
            def downstream(i):
                x, y = divmod(i, n)
                move = 1 if c % 2 == 0 else -1
                x, y = ((x + move) % n, y) if c < 2 else (x, (y + move) % n)
                return x * n + y

            return [(i, downstream(i)) for i in range(n * n)]

        last = [lax.ppermute(one, "dp", along(i % COLORS)) for i, one in enumerate(far)]

        out = pl.pallas_call(
            functools.partial(spread, n, layers, wides),
            out_shape=whole_shape,
            in_specs=[ANY] * (WEIGHTS + WEIGHTS * COLORS),
            out_specs=[ANY] * WEIGHTS,
            scratch_shapes=[pltpu.VMEM((8, n, rows, cols), bf16), dma((8,)), dma((8,))],
            compiler_params=pltpu.CompilerParams(vmem_limit_bytes=8 << 20),
            cost_estimate=pl.CostEstimate(flops=1 << 28, bytes_accessed=96 << 20, transcendentals=0),
            name="spread",
        )(*whole, *far)
        new_m, new_v = [], []
        for k in range(WEIGHTS):
            block = pl.BlockSpec((1, rows, cols), (lambda l, c: (l, 0, c)) if wides[k] else (lambda l, c: (l, c, 0)))
            one_m, one_v = pl.pallas_call(
                new_moments,
                grid=(layers, COLORS),
                out_shape=[jax.ShapeDtypeStruct(m[k].shape, f32)] * 2,
                in_specs=[pl.BlockSpec((1, 1, rows, cols), lambda l, c, k=k: (c, k * layers + l, 0, 0)), block, block],
                out_specs=[block, block],
                compiler_params=pltpu.CompilerParams(vmem_limit_bytes=8 << 20),
                cost_estimate=pl.CostEstimate(flops=1 << 25, bytes_accessed=12 << 20, transcendentals=0),
                name="moments",
            )(total, m[k], v[k])
            new_m.append(one_m)
            new_v.append(one_v)
        whole = []
        for k in range(WEIGHTS):
            done = pl.pallas_call(
                functools.partial(finish, n, layers, wides[k]),
                out_shape=whole_shape[k],
                in_specs=[VMEM] * COLORS + [ANY],
                out_specs=ANY,
                scratch_shapes=[dma((layers, COLORS))],
                input_output_aliases={COLORS: 0},
                compiler_params=pltpu.CompilerParams(vmem_limit_bytes=8 << 20),
                name="finish",
            )(*last[k * COLORS : (k + 1) * COLORS], out[k])
            whole.append(done.reshape(weights[k].shape))
        return (*whole, *new_m, *new_v)

    all_of, cut = P(None, None, None), P(None, "dp", None)
    return jax.shard_map(
        step,
        mesh=mesh,
        in_specs=(P(("rep", "dp"), None, None, None),) * 3 + (all_of,) * 3 + (cut,) * 6,
        out_specs=(P("rep", None, None),) * 3 + (P("rep", "dp", None),) * 6,
        check_vma=False,
    )
```

```python
import functools
import math

import jax
import jax.numpy as jnp
from jax import lax
from jax.experimental import pallas as pl
from jax.experimental.pallas import tpu as pltpu
from jax.sharding import PartitionSpec as P


MESH = pl.DeviceIdType.MESH
HBM = pl.BlockSpec(memory_space=pltpu.HBM)
WEIGHTS = 3
COLORS = 4
SLOTS = 3
SMALL = 8
DEPTH = 8
STAGGER_NS = 16000


class Grid:
    def __init__(self, n):
        me = lax.axis_index("dp")
        self.n, self.x, self.y = n, lax.div(me, n), lax.rem(me, n)
        self.me = me

    def sign(self, c):
        return 1 if c % 2 == 0 else -1

    def first(self, c):
        return self.x if c < 2 else self.y

    def second(self, c):
        return self.y if c < 2 else self.x

    def back(self, at, c, steps):
        return lax.rem(at + (2 * self.n - self.sign(c) * steps), self.n)

    def on(self, c, second):
        along_x = (c < 2) != second
        x, y = self.x, self.y
        if along_x:
            x = self.back(x, c, -1)
        else:
            y = self.back(y, c, -1)
        return {"dp": x * self.n + y}


def slab(ref, wide, layer, c, first, cols):
    owners = (first, slice(None)) if c < 2 else (slice(None), first)
    if wide:
        return ref.at[(layer, *owners, slice(None), pl.ds(c * cols, cols))]
    return ref.at[(layer, *owners, c)]


def piece(ref, wide, layer, c, first, second, cols):
    owner = (first, second) if c < 2 else (second, first)
    if wide:
        return ref.at[(layer, *owner, slice(None), pl.ds(c * cols, cols))]
    return ref.at[(layer, *owner, c)]


def mine(ref, wide, layer, c, cols):
    return ref.at[layer, :, pl.ds(c * cols, cols)] if wide else ref.at[layer, c]


def moments(m, v, g):
    return 0.9 * m + 0.1 * g, 0.95 * v + 0.05 * g * g


def adamw(w, m, v, g):
    m, v = moments(m, v, g)
    step = m * lax.rsqrt(v + 1e-8) + 0.1 * w
    return (w - 0.02 * step).astype(jnp.bfloat16)


def chunks_of(layers):
    units = [(k, layer) for k in range(WEIGHTS) for layer in range(layers)]
    half = len(units) // 2
    return [units[:half], units[half:-1], units[-1:]]


def far_part(far, layers, k, layer, c):
    for i, chunk in enumerate(chunks_of(layers)):
        if (k, layer) in chunk:
            return far[i * COLORS + c].at[chunk.index((k, layer))]


def exchange(n, layers, wides, *refs):
    g, w, m, v = (refs[i * WEIGHTS : (i + 1) * WEIGHTS] for i in range(4))
    refs = refs[4 * WEIGHTS :]
    whole, refs = refs[:WEIGHTS], refs[WEIGHTS:]
    count = len(chunks_of(layers)) * COLORS
    far, refs = refs[:count], refs[count:]
    total, got1, got2, refs = *refs[:3], refs[3:]
    a, b, s, a2, b2, c2, s2, gb, wb, wo, mo, vo, refs = *refs[:12], refs[12:]
    send1, recv1, send2, recv2, gsend1, grecv1, gsend2, grecv2, la, lb, la2, lb2, lc2, lg, lw, lo = refs

    rows, cols = gb.shape[2:]
    here = Grid(n)
    units = [(k, layer) for k in range(WEIGHTS) for layer in range(layers)]
    U = len(units)
    colors = range(COLORS)

    barrier = pltpu.get_barrier_semaphore()
    for c in colors:
        pl.semaphore_signal(barrier, inc=1, device_id=here.on(c, False), device_id_type=MESH)
    pl.semaphore_wait(barrier, COLORS)

    @pl.when(lax.rem(lax.axis_index("rep"), 2) == 1)
    def _():
        pl.delay(STAGGER_NS)


    def to(src, dst, send, recv, c, second):
        return pltpu.make_async_remote_copy(src, dst, send, recv, device_id=here.on(c, second), device_id_type=MESH)

    def g_slab(u, c, steps):
        k, layer = units[u]
        return slab(g[k], wides[k], layer, c, here.back(here.first(c), c, steps), cols)

    def g_piece(u, c, steps):
        k, layer = units[u]
        return piece(g[k], wides[k], layer, c, here.first(c), here.back(here.second(c), c, steps), cols)

    def w_slab(u, c, steps):
        k, layer = units[u]
        return slab(whole[k], wides[k], layer, c, here.back(here.first(c), c, steps), cols)

    def w_piece(u, c, steps):
        k, layer = units[u]
        return piece(whole[k], wides[k], layer, c, here.first(c), here.back(here.second(c), c, steps), cols)

    def hop1(t, u, c, src):
        return to(src, got1.at[c, t, u], send1.at[c, t, u], recv1.at[c, t, u], c, False)

    def hop2(t, u, c, src):
        return to(src, got2.at[c, t, u], send2.at[c, t, u], recv2.at[c, t, u], c, True)

    for u in range(U):
        for c in colors:
            hop1(0, u, c, g_slab(u, c, 1)).start()

    own = []
    for u, (k, layer) in enumerate(units):
        for c in colors:
            own.append(pltpu.make_async_copy(mine(m[k], wides[k], layer, c, cols), mo.at[c, u], lo.at[0, c, u]))
            own.append(pltpu.make_async_copy(mine(v[k], wides[k], layer, c, cols), vo.at[c, u], lo.at[1, c, u]))
            owner = piece(w[k], wides[k], layer, c, here.first(c), here.second(c), cols)
            own.append(pltpu.make_async_copy(owner, wo.at[c, u], lo.at[2, c, u]))

    def load_b(r, t, u, c):
        return pltpu.make_async_copy(g_slab(u, c, 1 + t), b.at[r % 2, c], lb.at[r % 2, c])

    rounds = [(t, u) for t in range(1, n - 1) for u in range(U)]
    for c in colors:
        load_b(0, *rounds[0], c).start()
    for copy in own:
        copy.start()
    for r, (t, u) in enumerate(rounds):
        loads = [pltpu.make_async_copy(got1.at[c, t - 1, u], a.at[c], la.at[c]) for c in colors]
        for c in colors:
            hop1(t - 1, u, c, got1.at[c, t - 1, u]).wait_recv()
            loads[c].start()
        if r + 1 < len(rounds):
            for c in colors:
                load_b(r + 1, *rounds[r + 1], c).start()
        slot = r % SLOTS
        for c in colors:
            loads[c].wait()
            load_b(r, t, u, c).wait()
            if r >= SLOTS:
                before = rounds[r - SLOTS]
                hop1(*before, c, s.at[slot, c]).wait_send()

            @pl.loop(0, n)
            def _(j):
                @pl.loop(0, rows, step=8)
                def _(i):
                    at = pl.ds(pl.multiple_of(i, 8), 8)
                    both = a[c, j, at, :].astype(jnp.float32) + b[r % 2, c, j, at, :].astype(jnp.float32)
                    s[slot, c, j, at, :] = both.astype(jnp.bfloat16)

        for c in colors:
            hop1(t, u, c, s.at[slot, c]).start()

    def load_b2(r, t, u, c):
        return pltpu.make_async_copy(g_piece(u, c, 1 + t), b2.at[r % 2, c], lb2.at[r % 2, c])

    def load_c2(r, t, u, c):
        return pltpu.make_async_copy(
            got1.at[c, n - 2, u, here.back(here.second(c), c, 1 + t)], c2.at[r % 2, c], lc2.at[r % 2, c]
        )

    def keep(u, c):
        return pltpu.make_async_copy(gb.at[c, u], total.at[c, u], lg.at[c, u])

    def place(u, c):
        return pltpu.make_async_copy(wb.at[c, u], w_piece(u, c, 0), lw.at[c, u])

    def gather1(t, u, c):
        return to(wb.at[c, u] if t == 0 else w_piece(u, c, t), w_piece(u, c, t), gsend1.at[c, t, u], grecv1.at[c, t, u], c, True)

    rounds = [(t, u) for t in range(n) for u in range(U)]
    for c in colors:
        load_b2(0, *rounds[0], c).start()
    for r, (t, u) in enumerate(rounds):
        par, slot = r % 2, r % SMALL
        for c in colors:
            if t == 0:
                hop1(n - 2, u, c, got1.at[c, n - 2, u]).wait_recv()
                load_c2(r, t, u, c).start()
            else:
                hop2(t - 1, u, c, got2.at[c, t - 1, u]).wait_recv()
                pltpu.make_async_copy(got2.at[c, t - 1, u], a2.at[c], la2.at[c]).start()
        if r + 1 < len(rounds):
            for c in colors:
                load_b2(r + 1, *rounds[r + 1], c).start()
                if rounds[r + 1][0] > 0:
                    load_c2(r + 1, *rounds[r + 1], c).start()
        for c in colors:
            load_b2(r, t, u, c).wait()
            load_c2(r, t, u, c).wait()
            if t > 0:
                pltpu.make_async_copy(got2.at[c, t - 1, u], a2.at[c], la2.at[c]).wait()
            if t < n - 1 and r >= SMALL:
                hop2(*rounds[r - SMALL], c, s2.at[slot, c]).wait_send()
            if t == n - 1:
                for copy in own[3 * (u * COLORS + c) : 3 * (u * COLORS + c) + 3]:
                    copy.wait()

            @pl.loop(0, rows, step=8)
            def _(i):
                at = pl.ds(pl.multiple_of(i, 8), 8)
                so_far = b2[par, c, at, :].astype(jnp.float32) + c2[par, c, at, :].astype(jnp.float32)
                if t > 0:
                    so_far = so_far + a2[c, at, :].astype(jnp.float32)
                summed = so_far.astype(jnp.bfloat16)
                if t < n - 1:
                    s2[slot, c, at, :] = summed
                else:
                    gb[c, u, at, :] = summed
                    wb[c, u, at, :] = adamw(
                        wo[c, u, at, :].astype(jnp.float32), mo[c, u, at, :], vo[c, u, at, :], summed.astype(jnp.float32)
                    )

        for c in colors:
            if t < n - 1:
                hop2(t, u, c, s2.at[slot, c]).start()
            else:
                gather1(0, u, c).start()
                place(u, c).start()
                keep(u, c).start()

    def got_piece(t, u, c):
        at = w_piece(u, c, 1 + t)
        return to(at, at, gsend1.at[c, t, u], grecv1.at[c, t, u], c, True)

    def gather2(t, u, c):
        k, layer = units[u]
        at = w_slab(u, c, t)
        there = at if t < n - 3 else far_part(far, layers, k, layer, c)
        return to(at, there, gsend2.at[c, t, u], grecv2.at[c, t, u], c, False)

    def got_slab(t, u, c):
        k, layer = units[u]
        at = w_slab(u, c, 1 + t) if t < n - 3 else far_part(far, layers, k, layer, c)
        return to(at, at, gsend2.at[c, t, u], grecv2.at[c, t, u], c, False)

    for t in range(1, n - 1):
        for u in range(U):
            for c in colors:
                got_piece(t - 1, u, c).wait_recv()
                gather1(t, u, c).start()
    for t in range(n - 2):
        for u in range(U):
            for c in colors:
                if t == 0:
                    place(u, c).wait()
                    got_piece(n - 2, u, c).wait_recv()
                else:
                    got_slab(t - 1, u, c).wait_recv()
                gather2(t, u, c).start()

    for u in range(U):
        for c in colors:
            keep(u, c).wait()
            hop1(0, u, c, g_slab(u, c, 1)).wait_send()
            for t in range(n - 1):
                gather1(t, u, c).wait_send()
            for t in range(n - 2):
                gather2(t, u, c).wait_send()
    for t, u in [(t, u) for t in range(1, n - 1) for u in range(U)][-SLOTS:]:
        for c in colors:
            hop1(t, u, c, s.at[0, c]).wait_send()
    first = len([1 for t, u in rounds if t < n - 1])
    waited = {rounds[r - SMALL] for r in range(SMALL, first)}
    for t, u in rounds[:first]:
        if (t, u) not in waited:
            for c in colors:
                hop2(t, u, c, s2.at[0, c]).wait_send()
    for u in range(U):
        for c in colors:
            got_slab(n - 3, u, c).wait_recv()


def spread(n, layers, wides, *refs):
    whole, refs = refs[:WEIGHTS], refs[WEIGHTS:]
    count = len(chunks_of(layers)) * COLORS
    far, refs = refs[:count], refs[count:]
    out, (buf, load_sem, store_sem) = refs[:WEIGHTS], refs[WEIGHTS:]
    slots, cols = buf.shape[0], buf.shape[-1]
    here = Grid(n)
    jobs = []
    for k in range(WEIGHTS):
        for layer in range(layers):
            for c in range(COLORS):
                for t in range(n - 1):
                    at = here.back(here.first(c), c, t)
                    dst = slab(out[k], wides[k], layer, c, at, cols)
                    src = slab(whole[k], wides[k], layer, c, at, cols) if t < n - 2 else far_part(far, layers, k, layer, c)
                    jobs.append((src, dst))

    def load(i):
        return pltpu.make_async_copy(jobs[i][0], buf.at[i % slots], load_sem.at[i % slots])

    def store(i):
        return pltpu.make_async_copy(buf.at[i % slots], jobs[i][1], store_sem.at[i % slots])

    lag = slots // 2
    for i in range(len(jobs) + lag):
        if i < len(jobs):
            if i >= slots:
                store(i - slots).wait()
            load(i).start()
        if i >= lag:
            load(i - lag).wait()
            store(i - lag).start()
    for i in range(len(jobs) - slots, len(jobs)):
        store(i).wait()


def finish(n, chunk, wides, *refs):
    weights = sorted({k for k, _ in chunk})
    last, (*out, _, buf, load_sem, store_sem) = refs[:COLORS], refs[COLORS + len(weights) + 1 :]
    here = Grid(n)
    loads, stores = [], []
    for i, (k, layer) in enumerate(chunk):
        for c in range(COLORS):
            at = here.back(here.first(c), c, n - 1)
            dst = slab(out[weights.index(k)], wides[k], layer, c, at, last[c].shape[-1])
            loads.append(pltpu.make_async_copy(last[c].at[i], buf.at[i, c], load_sem.at[i, c]))
            stores.append(pltpu.make_async_copy(buf.at[i, c], dst, store_sem.at[i, c]))
    for load in loads:
        load.start()
    for load, store in zip(loads, stores, strict=True):
        load.wait()
        store.start()
    for store in stores:
        store.wait()


def new_moments(layers, wides, total, *refs):
    m, v, m_out, v_out, refs = *(refs[i * WEIGHTS : (i + 1) * WEIGHTS] for i in range(4)), refs[4 * WEIGHTS :]
    gb, mb, vb, load_sem, store_sem = refs
    slots, rows, cols = gb.shape
    jobs = [(k, layer, c) for k in range(WEIGHTS) for layer in range(layers) for c in range(COLORS)]

    def loads(i):
        (k, layer, c), slot = jobs[i], i % slots
        pairs = (
            (total.at[c, k * layers + layer], gb),
            (mine(m[k], wides[k], layer, c, cols), mb),
            (mine(v[k], wides[k], layer, c, cols), vb),
        )
        return [pltpu.make_async_copy(src, dst.at[slot], load_sem.at[slot, q]) for q, (src, dst) in enumerate(pairs)]

    def stores(i):
        (k, layer, c), slot = jobs[i], i % slots
        pairs = ((mb, mine(m_out[k], wides[k], layer, c, cols)), (vb, mine(v_out[k], wides[k], layer, c, cols)))
        return [pltpu.make_async_copy(src.at[slot], dst, store_sem.at[slot, q]) for q, (src, dst) in enumerate(pairs)]

    lag = slots // 2
    for i in range(len(jobs) + lag):
        if i < len(jobs):
            if i >= slots:
                for copy in stores(i - slots):
                    copy.wait()
            for copy in loads(i):
                copy.start()
        if i >= lag:
            slot = (i - lag) % slots
            for copy in loads(i - lag):
                copy.wait()

            @pl.loop(0, rows, step=8)
            def _(row):
                at = pl.ds(pl.multiple_of(row, 8), 8)
                one_m, one_v = moments(mb[slot, at, :], vb[slot, at, :], gb[slot, at, :].astype(jnp.float32))
                mb[slot, at, :] = one_m
                vb[slot, at, :] = one_v

            for copy in stores(i - lag):
                copy.start()
    for i in range(len(jobs) - slots, len(jobs)):
        for copy in stores(i):
            copy.wait()


def solution(mesh):
    n = math.isqrt(mesh.shape["dp"])

    def step(*arrays):
        terms, weights, m, v = (arrays[i : i + WEIGHTS] for i in range(0, 4 * WEIGHTS, WEIGHTS))
        layers = m[0].shape[0]
        rows = min(one.shape[1] for one in m)
        cols = min(one.shape[2] for one in m)
        wides = [one.shape[2] != cols for one in m]
        units = WEIGHTS * layers

        def blocks(one, wide):
            return one.reshape((layers, n, n, rows, COLORS * cols) if wide else (layers, n, n, COLORS, rows, cols))

        def own(one, wide):
            return one if wide else one.reshape(layers, COLORS, rows, cols)

        views = [blocks(one[0], wide) for one, wide in zip(terms, wides, strict=True)]
        views += [blocks(one, wide) for one, wide in zip(weights, wides, strict=True)]
        views += [own(one, wide) for one, wide in zip(m + v, wides + wides, strict=True)]
        bf16, f32 = jnp.bfloat16, jnp.float32
        dma = pltpu.SemaphoreType.DMA
        whole_shape = [jax.ShapeDtypeStruct(one.shape, bf16) for one in views[WEIGHTS : 2 * WEIGHTS]]
        chunks = chunks_of(layers)
        far_shape = [jax.ShapeDtypeStruct((len(chunk), n, rows, cols), bf16) for chunk in chunks for _ in range(COLORS)]
        far_count = len(far_shape)
        results = pl.pallas_call(
            functools.partial(exchange, n, layers, wides),
            out_shape=(
                *whole_shape,
                *far_shape,
                jax.ShapeDtypeStruct((COLORS, units, rows, cols), bf16),
                jax.ShapeDtypeStruct((COLORS, n - 1, units, n, rows, cols), bf16),
                jax.ShapeDtypeStruct((COLORS, n - 1, units, rows, cols), bf16),
            ),
            in_specs=[HBM] * len(views),
            out_specs=[HBM] * (WEIGHTS + far_count + 3),
            scratch_shapes=[
                pltpu.VMEM((COLORS, n, rows, cols), bf16),
                pltpu.VMEM((2, COLORS, n, rows, cols), bf16),
                pltpu.VMEM((SLOTS, COLORS, n, rows, cols), bf16),
                pltpu.VMEM((COLORS, rows, cols), bf16),
                pltpu.VMEM((2, COLORS, rows, cols), bf16),
                pltpu.VMEM((2, COLORS, rows, cols), bf16),
                pltpu.VMEM((SMALL, COLORS, rows, cols), bf16),
                pltpu.VMEM((COLORS, units, rows, cols), bf16),
                pltpu.VMEM((COLORS, units, rows, cols), bf16),
                pltpu.VMEM((COLORS, units, rows, cols), bf16),
                pltpu.VMEM((COLORS, units, rows, cols), f32),
                pltpu.VMEM((COLORS, units, rows, cols), f32),
                dma((COLORS, n - 1, units)),
                dma((COLORS, n - 1, units)),
                dma((COLORS, n - 1, units)),
                dma((COLORS, n - 1, units)),
                dma((COLORS, n - 1, units)),
                dma((COLORS, n - 1, units)),
                dma((COLORS, n - 2, units)),
                dma((COLORS, n - 2, units)),
                dma((COLORS,)),
                dma((2, COLORS)),
                dma((COLORS,)),
                dma((2, COLORS)),
                dma((2, COLORS)),
                dma((COLORS, units)),
                dma((COLORS, units)),
                dma((3, COLORS, units)),
            ],
            compiler_params=pltpu.CompilerParams(collective_id=0, has_side_effects=True, vmem_limit_bytes=62 << 20),
            name="exchange",
        )(*views)
        whole, far, total = results[:WEIGHTS], results[WEIGHTS : WEIGHTS + far_count], results[-3]

        def along(c):
            def downstream(i):
                x, y = divmod(i, n)
                move = 1 if c % 2 == 0 else -1
                x, y = ((x + move) % n, y) if c < 2 else (x, (y + move) % n)
                return x * n + y

            return [(i, downstream(i)) for i in range(n * n)]

        last = [lax.ppermute(one, "dp", along(i % COLORS)) for i, one in enumerate(far)]

        out = pl.pallas_call(
            functools.partial(spread, n, layers, wides),
            out_shape=whole_shape,
            in_specs=[HBM] * (WEIGHTS + far_count),
            out_specs=[HBM] * WEIGHTS,
            scratch_shapes=[pltpu.VMEM((DEPTH, n, rows, cols), bf16), dma((DEPTH,)), dma((DEPTH,))],
            compiler_params=pltpu.CompilerParams(vmem_limit_bytes=62 << 20),
            cost_estimate=pl.CostEstimate(flops=1 << 28, bytes_accessed=96 << 20, transcendentals=0),
            name="spread",
        )(*whole, *far)
        moved = pl.pallas_call(
            functools.partial(new_moments, layers, wides),
            out_shape=[jax.ShapeDtypeStruct(one.shape, f32) for one in views[2 * WEIGHTS :]],
            in_specs=[HBM] * (1 + 2 * WEIGHTS),
            out_specs=[HBM] * (2 * WEIGHTS),
            scratch_shapes=[
                pltpu.VMEM((DEPTH, rows, cols), bf16),
                pltpu.VMEM((DEPTH, rows, cols), f32),
                pltpu.VMEM((DEPTH, rows, cols), f32),
                dma((DEPTH, 3)),
                dma((DEPTH, 2)),
            ],
            compiler_params=pltpu.CompilerParams(vmem_limit_bytes=62 << 20),
            cost_estimate=pl.CostEstimate(flops=1 << 26, bytes_accessed=36 << 20, transcendentals=0),
            name="moments",
        )(total, *views[2 * WEIGHTS :])
        new = [one.reshape(was.shape) for one, was in zip(moved, m + v, strict=True)]
        whole, before = list(out), new[0]
        for i, chunk in enumerate(chunks):
            ks = sorted({k for k, _ in chunk})
            *done, before = pl.pallas_call(
                functools.partial(finish, n, chunk, wides),
                out_shape=[*(whole_shape[k] for k in ks), jax.ShapeDtypeStruct((8, 128), f32)],
                in_specs=[HBM] * (COLORS + len(ks) + 1),
                out_specs=[HBM] * (len(ks) + 1),
                scratch_shapes=[
                    pltpu.VMEM((len(chunk), COLORS, n, rows, cols), bf16),
                    dma((len(chunk), COLORS)),
                    dma((len(chunk), COLORS)),
                ],
                input_output_aliases={COLORS + at: at for at in range(len(ks))},
                compiler_params=pltpu.CompilerParams(vmem_limit_bytes=62 << 20),
                name="finish",
            )(*last[i * COLORS : (i + 1) * COLORS], *(whole[k] for k in ks), before)
            for k, one in zip(ks, done, strict=True):
                whole[k] = one
        return (*(one.reshape(was.shape) for one, was in zip(whole, weights, strict=True)), *new)

    all_of, cut = P(None, None, None), P(None, "dp", None)
    return jax.shard_map(
        step,
        mesh=mesh,
        in_specs=(P(("rep", "dp"), None, None, None),) * 3 + (all_of,) * 3 + (cut,) * 6,
        out_specs=(P("rep", None, None),) * 3 + (P("rep", "dp", None),) * 6,
        check_vma=False,
    )
```
